32 devices in a mesh: front: 2 (over core), row: 4 (over y, x), col: 4 (over z).
Axes of the slice: x: 2, y: 2, z: 4, core: 2. Of those that a mesh axis runs over, the one named last changes fastest.
Arguments:
- front_rows: float32 [4096, 24576], P(('front', 'row'), 'col'), parts along dimension 0, may hold values from -0.0546875 to 0.0546875
- random_columns: bfloat16 [49152, 512], P(('front', 'col'), 'row'), parts along dimension 0, may hold values from -6 to 6
Outputs:
- basis: float32 [4096, 256], P(('front', 'row', 'col')), parts along dimension 0
- projected: float32 [1024, 512], P(('front', 'row')), parts along dimension 0
The draws below stay inside these ranges and needn't reach their ends.
There are 2 independent parts, one for each index of `front`. The reference program is written for one: setup_inputs(seed, part) draws one part's arguments, and reference() takes and returns one part's arrays. A program takes and returns all parts, laid end to end along the dimension named above; each array names one. Nothing has to cross between parts.
All inputs are finite; a program needn't handle non-finite values.
Results may differ from the reference program's by a relative error of at most 0.0003.
Values may be sent and summed in bfloat16 or wider, within the bound.
A program may use at most 64 MiB of HBM per device.

```python
import jax
import jax.numpy as jnp
from jax import lax

ORDER = 24576
SAMPLES = 512
LEAF = 1024
RANK = 256
ROWS = 2048


def raised(entries, own_key, source, target, blocks, factor):
    owner, partner = [(jnp.arange(entries.shape[position]) // (entries.shape[position] // blocks)).reshape([-1 if axis == position else 1 for axis in range(entries.ndim)]) for position in (source, target)]
    chosen = jax.random.permutation(own_key, blocks)[partner]
    strong = (owner == chosen) | (owner == (partner + blocks // 2) % blocks)
    return jnp.where(strong, factor * entries, entries)


def steps_of(stream_key, shape, shards, least, top_value):
    factor_of = 1.0
    for axis_at, parts in shards:
        heights = jax.random.uniform(jax.random.fold_in(jax.random.fold_in(stream_key, 6), axis_at), (parts,), jnp.float32, least / len(shards), top_value / len(shards))
        factor_of = factor_of * jnp.repeat(jnp.exp(heights), shape[axis_at] // parts).reshape((-1,) + (1,) * (len(shape) - 1 - axis_at))
    return factor_of


def centred(stream_key, extent, deviation, bound, shards=(), kind=jnp.bfloat16):
    factor_of = steps_of(stream_key, extent, shards, -0.22, 0.18) if shards else 1.0
    array = jax.random.normal(stream_key, extent, jnp.float32) * deviation * factor_of
    return jnp.minimum(jnp.maximum(array, -bound), bound).astype(kind)


def bell_draw_with(rng, dims, deviation, most, pieces, heavy, kind=jnp.bfloat16):
    drawn = deviation * jax.random.normal(rng, dims, jnp.float32)
    if pieces:
        drawn = drawn * steps_of(rng, dims, pieces, -0.22, 0.18)
    return jnp.clip(raised(drawn, jax.random.fold_in(rng, 3), *heavy), -most, most).astype(kind)


def setup_inputs(seed: int = 0, part: int = 0) -> dict:
    seeds = jax.random.split(jax.random.key(seed), 3)
    part_keys = jax.random.split(jax.random.fold_in(seeds[2], part), 3)
    front_rows = bell_draw_with(part_keys[0], (ROWS, ORDER), ORDER ** -0.5, 0.0546875, ((0, 4), (1, 4)), (1, 0, 4, 2.0), jnp.float32)
    random_columns = centred(part_keys[1], (ORDER, SAMPLES), 1.0, 6.0, ((0, 4), (1, 4)))
    return {"front_rows": front_rows, "random_columns": random_columns}


def reference(front_rows, random_columns):
    sketch = jnp.dot(front_rows.astype(jnp.float32), random_columns.astype(jnp.float32), precision=lax.Precision.HIGHEST, preferred_element_type=jnp.float32)
    count = ROWS // LEAF
    blocks = sketch.reshape(count, LEAF, SAMPLES)
    factor_q, factor_r = jnp.linalg.qr(blocks)
    diagonal = jnp.diagonal(factor_r, axis1=1, axis2=2)
    signs = jnp.where(diagonal < 0, -1.0, 1.0).astype(factor_r.dtype)
    factor_q = factor_q * signs[:, None, :]
    factor_r = factor_r * signs[:, :, None]
    basis = factor_q[:, :, :RANK].reshape(count * LEAF, RANK)
    projected = factor_r[:, :RANK, :].reshape(count * RANK, SAMPLES)
    return (basis, projected)
```

```python
import jax
import jax.numpy as jnp
from jax import lax
from jax.experimental import pallas as pl
from jax.experimental.pallas import tpu as pltpu
from jax.sharding import PartitionSpec as P

RANK = 256
PANEL = 8


def partner(value, axis, mask):
    pairs = [(source, source ^ mask) for source in range(lax.axis_size(axis))]
    return lax.ppermute(value, axis, pairs)


def product(left, right, contract):
    return lax.dot_general(
        left,
        right,
        ((contract[:1], contract[1:]), ((), ())),
        precision=lax.Precision.HIGHEST,
        preferred_element_type=jnp.float32,
    )


def halves(value, bit):
    size = value.shape[0] // 2
    low, high = value[:size], value[size:]
    return jnp.where(bit == 0, low, high), jnp.where(bit == 0, high, low)


def summed(value, axis):
    index = lax.axis_index(axis)
    strides = []
    stride = 1
    while stride < lax.axis_size(axis):
        strides.append(stride)
        stride *= 2
    for stride in strides:
        keep, give = halves(value, index // stride % 2)
        value = keep + partner(give, axis, stride)
    for stride in reversed(strides):
        other = partner(value, axis, stride)
        first = index // stride % 2 == 0
        value = jnp.concatenate(
            [jnp.where(first, value, other), jnp.where(first, other, value)], 0
        )
    return value


def factor(block, work):
    size = block.shape[0]
    rows = lax.broadcasted_iota(jnp.int32, (size, size), 0)
    lanes = lax.broadcasted_iota(jnp.int32, (size, size), 1)
    work[:, :size] = block
    work[:, size:] = jnp.where(rows == lanes, 1.0, 0.0).astype(jnp.float32)
    row_of = lax.broadcasted_iota(jnp.int32, (PANEL, 1), 0)
    for start in range(0, size, PANEL):
        panel = work[start : start + PANEL, :]
        for step in range(PANEL):
            column = panel[:, start + step : start + step + 1]
            scale = lax.rsqrt(column[step : step + 1, :])
            pivot = panel[step : step + 1, :] * scale
            weight = jnp.where(row_of > step, column * scale, 0.0)
            panel = jnp.where(row_of == step, pivot, panel - weight * pivot)
        work[start : start + PANEL, :] = panel
        if start + PANEL < size:
            tall = jnp.transpose(panel[:, :size])
            rest = work[start + PANEL :, :]
            for step in range(PANEL):
                rest = rest - tall[start + PANEL :, step : step + 1] * panel[step : step + 1, :]
            work[start + PANEL :, :] = rest
    return jnp.where(rows <= lanes, work[:, :size], 0.0), work[:, size:]


def leaf_kernel(gram_ref, mine_ref, coupling_ref, basis_ref, work):
    half = RANK // 2
    mine = jnp.transpose(mine_ref[...])
    upper, inverse = factor(gram_ref[:half, :half], work)
    top = product(inverse, gram_ref[:half, half:], (1, 0))
    top_mine = product(inverse, mine[:half], (1, 0))
    coupling_ref[:half, :half] = upper
    coupling_ref[:half, half:] = top
    across = top[:, : RANK - half]
    low = gram_ref[half:, half:] - product(across, top, (0, 0))
    low_mine = mine[half:] - product(across, top_mine, (0, 0))
    upper, inverse = factor(low[:, : RANK - half], work)
    coupling_ref[half:, :half] = jnp.zeros((RANK - half, half), jnp.float32)
    coupling_ref[half:, half:RANK] = upper
    coupling_ref[half:, RANK:] = product(inverse, low[:, RANK - half :], (1, 0))
    basis_ref[:, :half] = jnp.transpose(top_mine)
    basis_ref[:, half:] = jnp.transpose(product(inverse, low_mine, (1, 0)))


def leaf_factor(gram, mine):
    return pl.pallas_call(
        leaf_kernel,
        out_shape=(
            jax.ShapeDtypeStruct(gram.shape, jnp.float32),
            jax.ShapeDtypeStruct(mine.shape, jnp.float32),
        ),
        in_specs=[pl.BlockSpec(memory_space=pltpu.VMEM)] * 2,
        out_specs=(pl.BlockSpec(memory_space=pltpu.VMEM),) * 2,
        scratch_shapes=[pltpu.VMEM((RANK // 2, RANK), jnp.float32)],
    )(gram, mine)


def per_device(front_rows, random_columns):
    block_rows = front_rows.shape[0]
    depth, width = random_columns.shape
    row_count = lax.axis_size("row")
    col_index = lax.axis_index("col")
    row_index = lax.axis_index("row")
    own_rows = block_rows // lax.axis_size("col")

    near = lax.reduce_precision(front_rows, 8, 7)
    high = near.astype(jnp.bfloat16)
    low = (front_rows - near).astype(jnp.bfloat16)

    def sketch_of(columns):
        return jnp.dot(
            high, columns, preferred_element_type=jnp.float32
        ) + jnp.dot(low, columns, preferred_element_type=jnp.float32)

    if row_count == 4:
        beside = partner(random_columns, "row", 1)
        above = partner(random_columns, "row", 2)
        first = partner(above[: depth // 2], "row", 1)
        second = partner(beside[depth // 2 :], "row", 2)
        blocks = [random_columns, beside, above, jnp.concatenate([first, second], 0)]
    else:
        blocks = [random_columns] + [
            partner(random_columns, "row", mask) for mask in range(1, row_count)
        ]
    whole = jnp.zeros((block_rows, row_count * width), jnp.float32)
    for mask, columns in enumerate(blocks):
        total = summed(sketch_of(columns), "col")
        whole = lax.dynamic_update_slice_in_dim(
            whole, total, (row_index ^ mask) * width, 1
        )
    local_gram = product(whole[:, :RANK], whole, (0, 0))
    mine = lax.dynamic_slice_in_dim(whole[:, :RANK], col_index * own_rows, own_rows, 0)
    gram = local_gram + partner(local_gram, "row", 1)
    coupling, basis = leaf_factor(gram, mine)
    half = RANK // 2
    projected = lax.dynamic_slice_in_dim(coupling, row_index % 2 * half, half, 0)
    return (basis, projected)


def solution(mesh):
    return jax.shard_map(
        per_device,
        mesh=mesh,
        in_specs=(P(("front", "row"), "col"), P(("front", "col"), "row")),
        out_specs=(P(("front", "row", "col"), None), P(("front", "row"), None)),
        check_vma=False,
    )
```
